32 devices in a mesh: seq: 16 (over z, x, core), chan: 2 (over y).
Axes of the slice: x: 2, y: 2, z: 4, core: 2. Of those that a mesh axis runs over, the one named last changes fastest.
Arguments:
- signal: bfloat16 [524288, 256], P('seq', 'chan'), parts along dimension 1, may hold values from -6 to 6
- gate_values: bfloat16 [524288, 256], P('seq', 'chan'), parts along dimension 1, may hold values from -4 to 4
- skip_gain: float32 [256], P('chan'), parts along dimension 0, may hold values from 0.25 to 2
- filter_spectrum: bfloat16 [2, 512, 1024, 256], P(None, 'seq', None, 'chan'), parts along dimension 3, may hold values from -4 to 4, as said below
Outputs:
- gated_output: bfloat16 [524288, 256], P('seq', 'chan'), parts along dimension 1
The draws below stay inside these ranges and needn't reach their ends.
There are 2 independent parts, one for each index of `chan`. The reference program is written for one: setup_inputs(seed, part) draws one part's arguments, and reference() takes and returns one part's arrays. A program takes and returns all parts, laid end to end along the dimension named above; each array names one. Nothing has to cross between parts.
Inputs may be any that keep to these rules, and one draw needn't show every extreme that they name: `filter_spectrum`: the spectrum of a real filter: the complex entry at frequency k equals the conjugate of the entry at frequency (524288 - k) mod 524288.
All inputs are finite; a program needn't handle non-finite values.
Results may differ from the reference program's by a relative error of at most 0.0085.
Values may be sent and summed in bfloat16 or wider, within the bound.
A program may use at most 256 MiB of HBM per device.

```python
import math
import jax
import jax.numpy as jnp
from jax import lax

OUTER = 1024
INNER = 512
CH = 128
SEQ = 524288


def draw_filter_spectrum(key, part):
    length = INNER * OUTER
    first_key = jax.random.fold_in(key, 11)
    base = jax.random.normal(first_key, (2, length, CH), jnp.float32)
    mirror = jnp.roll(jnp.flip(base, axis=1), 1, axis=1)
    real_part = (base[0] + mirror[0]) * 0.7071
    imag_part = (base[1] - mirror[1]) * 0.7071
    both = jnp.clip(jnp.stack([real_part, imag_part]), -4.0, 4.0)
    return both.reshape(2, INNER, OUTER, CH).astype(jnp.bfloat16)


def level_of(rng, extent, split, smallest, top_value):
    factor_of = 1.0
    for axis_at, blocks in split:
        heights = jax.random.uniform(jax.random.fold_in(jax.random.fold_in(rng, 6), axis_at), (blocks,), jnp.float32, smallest / len(split), top_value / len(split))
        factor_of = factor_of * jnp.repeat(jnp.exp(heights), extent[axis_at] // blocks).reshape((-1,) + (1,) * (len(extent) - 1 - axis_at))
    return factor_of


def centred(rng, extent, scale, limit, cuts=(), held_as=jnp.bfloat16):
    level = level_of(rng, extent, cuts, -0.22, 0.18) if cuts else 1.0
    values = jax.random.normal(rng, extent, jnp.float32) * scale * level
    return jnp.minimum(jnp.maximum(values, -limit), limit).astype(held_as)


def setup_inputs(seed: int = 0, part: int = 0) -> dict:
    keys = jax.random.split(jax.random.key(seed), 5)
    part_keys = jax.random.split(jax.random.fold_in(keys[4], part), 5)
    signal = centred(part_keys[0], (SEQ, CH), 1.0, 6.0, ((0, 16),))
    gate_values = centred(part_keys[1], (SEQ, CH), 1.0, 4.0, ((0, 16),))
    skip_gain = jnp.clip(jnp.exp(jax.random.uniform(part_keys[2], (CH,), jnp.float32, math.log(0.25), math.log(2.0))), 0.25, 2.0)
    filter_spectrum = draw_filter_spectrum(jax.random.fold_in(jax.random.fold_in(keys[4], part), 71), part)
    return {"signal": signal, "gate_values": gate_values, "skip_gain": skip_gain, "filter_spectrum": filter_spectrum}


def tables(length):
    indices = lax.iota(jnp.int32, length)
    angles = 2.0 * math.pi / length * (indices[:, None] * indices[None, :] % length).astype(jnp.float32)
    return (jnp.cos(angles).astype(jnp.bfloat16), jnp.sin(angles).astype(jnp.bfloat16))

def twiddle(c_values, b_values, length):
    angles = 2.0 * math.pi / length * (c_values[:, None] * b_values[None, :] % length).astype(jnp.float32)
    return (jnp.cos(angles), jnp.sin(angles))

def convolve(operands):
    pieces, filter_cols = operands
    cos_a, sin_a = tables(OUTER)
    cos_b, sin_b = tables(INNER)
    inner_table = jnp.stack([cos_b, sin_b]).astype(jnp.float32)
    tw_cos, tw_sin = twiddle(lax.iota(jnp.int32, OUTER), lax.iota(jnp.int32, INNER), SEQ)
    tw_cos = tw_cos[:, :, None]
    tw_sin = tw_sin[:, :, None]
    outer_scale = 1.0 / math.sqrt(OUTER)
    inner_scale = 1.0 / math.sqrt(INNER)
    breadth = pieces.shape[2]
    flattened = pieces.reshape(OUTER, INNER * breadth)
    fwd_re = jnp.dot(cos_a, flattened, preferred_element_type=jnp.float32).reshape(OUTER, INNER, breadth)
    fwd_im = -jnp.dot(sin_a, flattened, preferred_element_type=jnp.float32).reshape(OUTER, INNER, breadth)
    twisted = jnp.stack([(fwd_re * tw_cos + fwd_im * tw_sin) * outer_scale, (fwd_im * tw_cos - fwd_re * tw_sin) * outer_scale]).astype(jnp.bfloat16)
    partials = jnp.einsum('tdb,scbk->tscdk', inner_table, twisted.astype(jnp.float32), precision=lax.Precision.HIGHEST)
    spectrum = jnp.stack([(partials[0, 0] + partials[1, 1]) * inner_scale, (partials[0, 1] - partials[1, 0]) * inner_scale]).astype(jnp.bfloat16)
    filter_re = jnp.swapaxes(filter_cols[0], 0, 1).astype(jnp.float32)
    filter_im = jnp.swapaxes(filter_cols[1], 0, 1).astype(jnp.float32)
    spec_re = spectrum[0].astype(jnp.float32)
    spec_im = spectrum[1].astype(jnp.float32)
    product = jnp.stack([spec_re * filter_re - spec_im * filter_im, spec_re * filter_im + spec_im * filter_re]).astype(jnp.bfloat16)
    partials = jnp.einsum('tbd,scdk->tscbk', inner_table, product.astype(jnp.float32), precision=lax.Precision.HIGHEST)
    back_re = (partials[0, 0] - partials[1, 1]) * inner_scale
    back_im = (partials[0, 1] + partials[1, 0]) * inner_scale
    rotated_re = (back_re * tw_cos - back_im * tw_sin).astype(jnp.bfloat16)
    rotated_im = (back_re * tw_sin + back_im * tw_cos).astype(jnp.bfloat16)
    convolved = (jnp.dot(cos_a, rotated_re.reshape(OUTER, INNER * breadth), preferred_element_type=jnp.float32) - jnp.dot(sin_a, rotated_im.reshape(OUTER, INNER * breadth), preferred_element_type=jnp.float32)) * outer_scale
    return convolved.reshape(OUTER, INNER, breadth).astype(jnp.bfloat16)

def reference(signal, gate_values, skip_gain, filter_spectrum):
    channels = signal.shape[1]
    group_width = 16 if channels % 16 == 0 else channels
    groups = channels // group_width
    signal_grid = signal.reshape(OUTER, INNER, groups, group_width).transpose(2, 0, 1, 3)
    filter_grid = filter_spectrum.reshape(2, INNER, OUTER, groups, group_width).transpose(3, 0, 1, 2, 4)
    convolved = lax.map(convolve, (signal_grid, filter_grid))
    convolved = convolved.transpose(1, 2, 0, 3).reshape(SEQ, channels)
    result = gate_values.astype(jnp.float32) * (convolved.astype(jnp.float32) + skip_gain[None, :].astype(jnp.float32) * signal.astype(jnp.float32))
    return result.astype(jnp.bfloat16)
```

```python
import functools
import math

import jax
import jax.numpy as jnp
from jax import lax
from jax.experimental import pallas as pl
from jax.experimental.pallas import tpu as pltpu
from jax.sharding import PartitionSpec as P

OUTER = 1024
INNER = 512
SEQ = 524288
MESH = pl.DeviceIdType.MESH


def tables(length):
    indices = lax.iota(jnp.int32, length)
    angles = (
        2.0 * math.pi / length * (indices[:, None] * indices[None, :] % length).astype(jnp.float32)
    )
    return (jnp.cos(angles).astype(jnp.bfloat16), jnp.sin(angles).astype(jnp.bfloat16))


def twiddle(c_values, b_values, length):
    angles = (
        2.0
        * math.pi
        / length
        * (c_values[:, None] * b_values[None, :] % length).astype(jnp.float32)
    )
    return (jnp.cos(angles), jnp.sin(angles))


def exchange(arrays, out_shape, moves, shards, collective_id):
    count = len(moves)

    def kernel(*refs):
        ins, out = refs[: len(arrays)], refs[len(arrays)]
        send_sem, recv_sem, own_sem = refs[len(arrays) + 1 :]
        me = lax.axis_index("seq")
        barrier = pltpu.get_barrier_semaphore()
        for i in range(1, shards):
            pl.semaphore_signal(
                barrier, inc=1, device_id={"seq": lax.rem(me + i, shards)}, device_id_type=MESH
            )
        pl.semaphore_wait(barrier, shards - 1)
        copies = []
        for i in range(1, shards):
            to = lax.rem(me + i, shards)
            for m, (which, take, put) in enumerate(moves):
                copies.append(
                    pltpu.make_async_remote_copy(
                        src_ref=ins[which].at[take(to)],
                        dst_ref=out.at[put(me)],
                        send_sem=send_sem.at[(i - 1) * count + m],
                        recv_sem=recv_sem.at[(i - 1) * count + m],
                        device_id={"seq": to},
                        device_id_type=MESH,
                    )
                )
                copies[-1].start()
        for m, (which, take, put) in enumerate(moves):
            copies.append(
                pltpu.make_async_copy(ins[which].at[take(me)], out.at[put(me)], own_sem.at[m])
            )
            copies[-1].start()
        for copy in copies:
            copy.wait()

    return pl.pallas_call(
        kernel,
        out_shape=jax.ShapeDtypeStruct(out_shape, jnp.bfloat16),
        in_specs=[pl.BlockSpec(memory_space=pl.ANY)] * len(arrays),
        out_specs=pl.BlockSpec(memory_space=pl.ANY),
        scratch_shapes=[
            pltpu.SemaphoreType.DMA(((shards - 1) * count,)),
            pltpu.SemaphoreType.DMA(((shards - 1) * count,)),
            pltpu.SemaphoreType.DMA((count,)),
        ],
        compiler_params=pltpu.CompilerParams(collective_id=collective_id, has_side_effects=True),
        name=f"exchange_{collective_id}",
    )(*arrays)


def block(index, size, base=0):
    return pl.ds(pl.multiple_of(base + index * size, math.gcd(base, size) if base else size), size)


def section_kernel(fwd_ref, inv_ref, q_ref, filter_ref, cos_ref, sin_ref, out_ref):
    group = q_ref.shape[0]
    half = q_ref.shape[1] // 2
    scale = 1.0 / math.sqrt(half)
    lanes = q_ref.shape[2]
    q = jnp.concatenate([q_ref[g] for g in range(group)], axis=-1)
    spectrum = jnp.dot(fwd_ref[...], q, preferred_element_type=jnp.float32)
    spectrum = (spectrum * scale).astype(jnp.bfloat16).astype(jnp.float32)
    spec_re, spec_im = spectrum[:half], spectrum[half:]
    filt = jnp.concatenate([filter_ref[g] for g in range(group)], axis=-1).astype(jnp.float32)
    filter_re, filter_im = filt[:half], filt[half:]
    product = jnp.concatenate(
        [spec_re * filter_re - spec_im * filter_im, spec_re * filter_im + spec_im * filter_re],
        axis=0,
    ).astype(jnp.bfloat16)
    back = jnp.dot(inv_ref[...], product, preferred_element_type=jnp.float32) * scale
    back_re, back_im = back[:half], back[half:]
    for g in range(group):
        cols = slice(g * lanes, (g + 1) * lanes)
        re, im = back_re[:, cols], back_im[:, cols]
        cos, sin = cos_ref[g], sin_ref[g]
        out_ref[g, :half] = (re * cos - im * sin).astype(jnp.bfloat16)
        out_ref[g, half:] = (re * sin + im * cos).astype(jnp.bfloat16)


def section(fwd, inv, q, filt, cos, sin):
    rows, depth, lanes = q.shape
    group = 2
    whole = pl.BlockSpec((depth, depth), lambda i: (0, 0))
    full = pl.BlockSpec((group, depth, lanes), lambda i: (i, 0, 0))
    part = pl.BlockSpec((group, depth // 2, lanes), lambda i: (i, 0, 0))
    return pl.pallas_call(
        section_kernel,
        grid=(pl.cdiv(rows, group),),
        in_specs=[whole, whole, full, full, part, part],
        out_specs=full,
        out_shape=jax.ShapeDtypeStruct(q.shape, jnp.bfloat16),
        compiler_params=pltpu.CompilerParams(vmem_limit_bytes=56 * 1024 * 1024),
        name="section",
    )(fwd, inv, q, filt, cos, sin)


def local(signal, gate_values, skip_gain, filter_spectrum):
    shards = lax.axis_size("seq")
    own_index = lax.axis_index("seq")
    channels = signal.shape[1]
    outer_loc = OUTER // shards
    inner_loc = INNER // shards
    c_loc = -(-(OUTER // 2 + 1) // shards)
    rows = c_loc * shards
    cos_a, sin_a = tables(OUTER)
    cos_b, sin_b = tables(INNER)
    outer_scale = 1.0 / math.sqrt(OUTER)
    fwd_b = jnp.concatenate(
        [jnp.concatenate([cos_b, sin_b], 1), jnp.concatenate([-sin_b, cos_b], 1)], 0
    )
    inv_b = jnp.concatenate(
        [jnp.concatenate([cos_b, -sin_b], 1), jnp.concatenate([sin_b, cos_b], 1)], 0
    )
    own_b = own_index * inner_loc + lax.iota(jnp.int32, inner_loc)
    own_c = own_index * c_loc + lax.iota(jnp.int32, c_loc)
    c_all = lax.iota(jnp.int32, rows)
    cols_cos, cols_sin = twiddle(c_all, own_b, SEQ)
    rows_cos, rows_sin = twiddle(own_c, lax.iota(jnp.int32, INNER), SEQ)
    cols_cos = cols_cos[:, :, None]
    cols_sin = cols_sin[:, :, None]
    spread = (c_loc, INNER, channels)
    rows_cos = jnp.broadcast_to(rows_cos[:, :, None], spread)
    rows_sin = jnp.broadcast_to(rows_sin[:, :, None], spread)
    every = slice(None)

    def lead(size, base=0):
        return lambda t: (block(t, size, base), every, every)

    def middle(size, base=0):
        return lambda t: (every, block(t, size, base), every)

    signal_grid = signal.reshape(outer_loc, INNER, channels)
    pieces = exchange(
        [signal_grid],
        (OUTER, inner_loc, channels),
        [(0, middle(inner_loc), lead(outer_loc))],
        shards,
        0,
    )
    filter_rows = jnp.swapaxes(filter_spectrum[:, :, :rows], 1, 2)
    filter_cols = exchange(
        [filter_rows[0], filter_rows[1]],
        (c_loc, 2 * INNER, channels),
        [
            (0, lead(c_loc), middle(inner_loc)),
            (1, lead(c_loc), middle(inner_loc, INNER)),
        ],
        shards,
        1,
    )
    flattened = pieces.reshape(OUTER, inner_loc * channels)
    shape = (rows, inner_loc, channels)
    fwd_re = jnp.dot(cos_a[:rows], flattened, preferred_element_type=jnp.float32).reshape(shape)
    fwd_im = -jnp.dot(sin_a[:rows], flattened, preferred_element_type=jnp.float32).reshape(shape)
    q_re = ((fwd_re * cols_cos + fwd_im * cols_sin) * outer_scale).astype(jnp.bfloat16)
    q_im = ((fwd_im * cols_cos - fwd_re * cols_sin) * outer_scale).astype(jnp.bfloat16)
    q = exchange(
        [q_re, q_im],
        (c_loc, 2 * INNER, channels),
        [
            (0, lead(c_loc), middle(inner_loc)),
            (1, lead(c_loc), middle(inner_loc, INNER)),
        ],
        shards,
        2,
    )
    rotated = section(fwd_b, inv_b, q, filter_cols, rows_cos, rows_sin)
    pieces = exchange(
        [rotated],
        (2 * rows, inner_loc, channels),
        [
            (0, middle(inner_loc), lead(c_loc)),
            (0, middle(inner_loc, INNER), lead(c_loc, rows)),
        ],
        shards,
        3,
    )
    weight = jnp.where((c_all == 0) | (c_all == OUTER // 2), 1.0, 2.0)
    weight = jnp.where(c_all > OUTER // 2, 0.0, weight).astype(jnp.bfloat16)[None, :]
    back_a = jnp.concatenate([cos_a[:, :rows] * weight, -sin_a[:, :rows] * weight], 1)
    convolved = (
        jnp.dot(
            back_a,
            pieces.reshape(2 * rows, inner_loc * channels),
            preferred_element_type=jnp.float32,
        )
        * outer_scale
    )
    by_columns = convolved.astype(jnp.bfloat16).reshape(OUTER, inner_loc, channels)
    convolved = exchange(
        [by_columns],
        (outer_loc, INNER, channels),
        [(0, lead(outer_loc), middle(inner_loc))],
        shards,
        4,
    ).reshape(outer_loc * INNER, channels)
    result = gate_values.astype(jnp.float32) * (
        convolved.astype(jnp.float32) + skip_gain[None, :] * signal.astype(jnp.float32)
    )
    return result.astype(jnp.bfloat16)


def solution(mesh):
    return jax.shard_map(
        local,
        mesh=mesh,
        in_specs=(P("seq", "chan"), P("seq", "chan"), P("chan"), P(None, "seq", None, "chan")),
        out_specs=P("seq", "chan"),
        check_vma=False,
    )
```

```python
import functools
import math

import jax
import jax.numpy as jnp
from jax import lax
from jax.experimental import pallas as pl
from jax.experimental.pallas import tpu as pltpu
from jax.sharding import PartitionSpec as P

OUTER = 1024
INNER = 512
SEQ = 524288
MESH = pl.DeviceIdType.MESH


def tables(length):
    indices = lax.iota(jnp.int32, length)
    angles = (
        2.0 * math.pi / length * (indices[:, None] * indices[None, :] % length).astype(jnp.float32)
    )
    return (jnp.cos(angles).astype(jnp.bfloat16), jnp.sin(angles).astype(jnp.bfloat16))


def twiddle(c_values, b_values, length):
    angles = (
        2.0
        * math.pi
        / length
        * (c_values[:, None] * b_values[None, :] % length).astype(jnp.float32)
    )
    return (jnp.cos(angles), jnp.sin(angles))


def exchange(arrays, out_shape, moves, shards, collective_id):
    count = len(moves)

    def kernel(*refs):
        ins, out = refs[: len(arrays)], refs[len(arrays)]
        send_sem, recv_sem, own_sem = refs[len(arrays) + 1 :]
        me = lax.axis_index("seq")
        barrier = pltpu.get_barrier_semaphore()
        for i in range(1, shards):
            pl.semaphore_signal(
                barrier, inc=1, device_id={"seq": lax.rem(me + i, shards)}, device_id_type=MESH
            )
        pl.semaphore_wait(barrier, shards - 1)
        copies = []
        for i in range(1, shards):
            to = lax.rem(me + i, shards)
            for m, (which, take, put) in enumerate(moves):
                copies.append(
                    pltpu.make_async_remote_copy(
                        src_ref=ins[which].at[take(to)],
                        dst_ref=out.at[put(me)],
                        send_sem=send_sem.at[(i - 1) * count + m],
                        recv_sem=recv_sem.at[(i - 1) * count + m],
                        device_id={"seq": to},
                        device_id_type=MESH,
                    )
                )
                copies[-1].start()
        for m, (which, take, put) in enumerate(moves):
            copies.append(
                pltpu.make_async_copy(ins[which].at[take(me)], out.at[put(me)], own_sem.at[m])
            )
            copies[-1].start()
        for copy in copies:
            copy.wait()

    return pl.pallas_call(
        kernel,
        out_shape=jax.ShapeDtypeStruct(out_shape, jnp.bfloat16),
        in_specs=[pl.BlockSpec(memory_space=pl.ANY)] * len(arrays),
        out_specs=pl.BlockSpec(memory_space=pl.ANY),
        scratch_shapes=[
            pltpu.SemaphoreType.DMA(((shards - 1) * count,)),
            pltpu.SemaphoreType.DMA(((shards - 1) * count,)),
            pltpu.SemaphoreType.DMA((count,)),
        ],
        compiler_params=pltpu.CompilerParams(collective_id=collective_id, has_side_effects=True),
        name=f"exchange_{collective_id}",
    )(*arrays)


def block(index, size, base=0):
    return pl.ds(pl.multiple_of(base + index * size, math.gcd(base, size) if base else size), size)


def local(signal, gate_values, skip_gain, filter_spectrum):
    shards = lax.axis_size("seq")
    channels = signal.shape[1]
    ch_loc = channels // shards
    outer_loc = OUTER // shards
    inner_loc = INNER // shards
    rows = -(-(OUTER // 2 + 1) // 16) * 16
    cos_a, sin_a = tables(OUTER)
    cos_b, sin_b = tables(INNER)
    outer_scale = 1.0 / math.sqrt(OUTER)
    inner_scale = 1.0 / math.sqrt(INNER)
    fwd_b = jnp.concatenate(
        [jnp.concatenate([cos_b, sin_b], 1), jnp.concatenate([-sin_b, cos_b], 1)], 0
    )
    inv_b = jnp.concatenate(
        [jnp.concatenate([cos_b, -sin_b], 1), jnp.concatenate([sin_b, cos_b], 1)], 0
    )
    c_all = lax.iota(jnp.int32, rows)
    cos, sin = twiddle(lax.iota(jnp.int32, INNER), c_all, SEQ)
    every = slice(None)

    def lead(size):
        return lambda t: (block(t, size), every, every)

    def middle(size):
        return lambda t: (every, block(t, size), every)

    grid = exchange(
        [signal.T.reshape(channels, outer_loc, INNER)],
        (ch_loc, OUTER, INNER),
        [(0, lead(ch_loc), middle(outer_loc))],
        shards,
        0,
    )
    filt = [
        exchange(
            [filter_spectrum[p, :, :rows].transpose(2, 0, 1)],
            (ch_loc, INNER, rows),
            [(0, lead(ch_loc), middle(inner_loc))],
            shards,
            1 + p,
        ).astype(jnp.float32)
        for p in range(2)
    ]
    fwd_re = jnp.einsum(
        "kab,ac->kbc", grid, cos_a[:, :rows], preferred_element_type=jnp.float32
    )
    fwd_im = -jnp.einsum(
        "kab,ac->kbc", grid, sin_a[:, :rows], preferred_element_type=jnp.float32
    )
    q = jnp.concatenate(
        [
            (fwd_re * cos + fwd_im * sin) * outer_scale,
            (fwd_im * cos - fwd_re * sin) * outer_scale,
        ],
        axis=1,
    ).astype(jnp.bfloat16)
    spectrum = jnp.einsum("db,kbc->kdc", fwd_b, q, preferred_element_type=jnp.float32)
    spectrum = (spectrum * inner_scale).astype(jnp.bfloat16).astype(jnp.float32)
    re, im = spectrum[:, :INNER], spectrum[:, INNER:]
    product = jnp.concatenate(
        [re * filt[0] - im * filt[1], re * filt[1] + im * filt[0]], axis=1
    ).astype(jnp.bfloat16)
    back = jnp.einsum("bd,kdc->kbc", inv_b, product, preferred_element_type=jnp.float32)
    back = back * inner_scale
    re, im = back[:, :INNER], back[:, INNER:]
    r_re = (re * cos - im * sin).astype(jnp.bfloat16)
    r_im = (re * sin + im * cos).astype(jnp.bfloat16)
    weight = jnp.where((c_all == 0) | (c_all == OUTER // 2), 1.0, 2.0)
    weight = jnp.where(c_all > OUTER // 2, 0.0, weight).astype(jnp.bfloat16)[None, :]
    convolved = (
        jnp.einsum(
            "ac,kbc->kab", cos_a[:, :rows] * weight, r_re, preferred_element_type=jnp.float32
        )
        - jnp.einsum(
            "ac,kbc->kab", sin_a[:, :rows] * weight, r_im, preferred_element_type=jnp.float32
        )
    ) * outer_scale
    convolved = exchange(
        [convolved.astype(jnp.bfloat16)],
        (channels, outer_loc, INNER),
        [(0, middle(outer_loc), lead(ch_loc))],
        shards,
        3,
    )
    convolved = convolved.reshape(channels, outer_loc * INNER).T
    result = gate_values.astype(jnp.float32) * (
        convolved.astype(jnp.float32) + skip_gain[None, :] * signal.astype(jnp.float32)
    )
    return result.astype(jnp.bfloat16)


def solution(mesh):
    return jax.shard_map(
        local,
        mesh=mesh,
        in_specs=(P("seq", "chan"), P("seq", "chan"), P("chan"), P(None, "seq", None, "chan")),
        out_specs=P("seq", "chan"),
        check_vma=False,
    )
```
